512 devices in a mesh: user: 32 (over z_hi, y, core), item: 16 (over x, z_lo).
Axes of the slice: x: 4, y: 4, z: 16 (z_hi: 4, z_lo: 4; z = z_hi * 4 + z_lo), core: 2. Of those that a mesh axis runs over, the one named last changes fastest.
Arguments:
- user_comps: bfloat16 [4096, 512], P(('user', 'item')), may hold values from -6 to 6
- item_text: bfloat16 [4096, 1024], P(('user', 'item')), may hold values from -6 to 6
- item_proj: bfloat16 [1024, 512], replicated, may hold values from -0.1875 to 0.1875
- w_in: float32 [64, 128], replicated, may hold values from -0.75 to 0.75
- b_in: float32 [128], replicated, may hold values from -4 to 4
- w_out: float32 [128, 64], replicated, may hold values from -1.5 to 1.5
- b_out: float32 [64], replicated, may hold values from -4 to 4
- pair_user: int32 [524288], P(('user', 'item')), may hold values from 0 to 127
- pair_item: int32 [524288], P(('user', 'item')), may hold values from 0 to 255
- teacher: float32 [524288], P(('user', 'item')), may hold values from -12 to 12
Outputs:
- user_grad: float32 [4096, 512], P(('user', 'item'))
- item_grad: float32 [4096, 512], P(('user', 'item'))
The draws below stay inside these ranges and needn't reach their ends.
Inputs may be any that keep to these rules, and one draw needn't show every extreme that they name: `pair_user`: index of a user among the 128 users of the pair's tile. `pair_item`: index of an item among the 256 items of the pair's tile.
All inputs are finite; a program needn't handle non-finite values.
Results may differ from the reference program's by a relative error of at most 0.0058.
Values may be sent and summed in bfloat16 or wider, within the bound.
A program may use at most 64 MiB of HBM per device.

```python
import math
import jax
import jax.numpy as jnp
from jax import lax

DT = 1024
COMPS = 8
CDIM = 64
GATE_HIDDEN = 128
USER_DEV = 128
ITEM_DEV = 256
PAIR_DEV = 1024
GATES = 64
USERS = 4096
ITEMS = 4096
ISUB = 8
PAIRS = 524288
N_USER = 32
N_ITEM = 16


def place_ends(drawn, rng, smallest, top_value):
    dims = drawn.shape
    spot = [jax.random.randint(jax.random.fold_in(rng, axis), (), 0, dims[axis]) for axis in range(len(dims))]
    drawn = drawn.at[tuple(spot)].set(smallest)
    longest = dims.index(max(dims))
    spot[longest] = (spot[longest] + 1) % dims[longest]
    return drawn.at[tuple(spot)].set(top_value)


def block_scale(key, extent, shards, least, top_value):
    def one(axis_at, parts):
        heights = jax.random.uniform(jax.random.fold_in(jax.random.fold_in(key, 6), axis_at), (parts,), jnp.float32, least / len(shards), top_value / len(shards))
        return jnp.repeat(jnp.exp(heights), extent[axis_at] // parts).reshape((-1,) + (1,) * (len(extent) - axis_at - 1))

    loudness = one(*shards[0])
    for cut in shards[1:]:
        loudness = loudness * one(*cut)
    return loudness


def noise(key, shape, deviation, bound, split=(), kind=jnp.bfloat16):
    drawn = deviation * jax.random.normal(key, shape, jnp.float32)
    if split:
        drawn = drawn * block_scale(key, shape, split, -0.22, 0.18)
    return jnp.clip(drawn, -bound, bound).astype(kind)


def setup_inputs(seed: int = 0) -> dict:
    splits = jax.random.split(jax.random.key(seed), 11)
    return {
        "user_comps": noise(splits[0], (USERS, COMPS * CDIM), 1.0, 6.0, ((0, 512),)),
        "item_text": noise(splits[1], (ITEMS, DT), 1.0, 6.0, ((0, 512),)),
        "item_proj": noise(splits[2], (DT, COMPS * CDIM), DT ** -0.5, 0.1875),
        "w_in": noise(splits[3], (GATES, GATE_HIDDEN), GATES ** -0.5, 0.75, (), jnp.float32),
        "b_in": noise(splits[4], (GATE_HIDDEN,), 1.0, 4.0, (), jnp.float32),
        "w_out": noise(splits[5], (GATE_HIDDEN, GATES), 16 ** -0.5, 1.5, (), jnp.float32),
        "b_out": noise(splits[6], (GATES,), 1.0, 4.0, (), jnp.float32),
        "pair_user": place_ends(jax.random.randint(splits[7], (PAIRS,), 0, USER_DEV), jax.random.fold_in(splits[7], 1), 0, USER_DEV - 1).astype(jnp.int32),
        "pair_item": place_ends(jax.random.randint(splits[8], (PAIRS,), 0, ITEM_DEV), jax.random.fold_in(splits[8], 1), 0, ITEM_DEV - 1).astype(jnp.int32),
        "teacher": noise(splits[9], (PAIRS,), 2.0, 12.0, ((0, 512),), jnp.float32),
    }


gate_cap = 8.0

def component_norm(values):
    mean_square = lax.optimization_barrier(jnp.mean(values * values, axis=-1, keepdims=True))
    return values * lax.rsqrt(mean_square + 1e-06)

def pair_grads(user_portion, item_portion, target, w_in, b_in, w_out, b_out, loss_scale):
    width = user_portion.shape[-1]
    reciprocal_norm = 1.0 / math.sqrt(width)
    user_broadcast = user_portion.astype(jnp.float32)
    item_broadcast = item_portion.astype(jnp.float32)
    mixture_logits = jnp.einsum('xvw,xzw->xvz', user_broadcast, item_broadcast, precision=lax.Precision.HIGHEST) * reciprocal_norm
    pair_count = mixture_logits.shape[0]
    flat_logits = mixture_logits.reshape(pair_count, -1)
    hidden_in = jnp.dot(flat_logits, w_in, precision=lax.Precision.HIGHEST) + b_in
    sig_pre = jax.nn.sigmoid(hidden_in)
    hidden = hidden_in * sig_pre
    gate_raw = jnp.dot(hidden, w_out, precision=lax.Precision.HIGHEST) + b_out
    capped = jnp.tanh(gate_raw / gate_cap)
    exp_gate = jnp.exp(gate_cap * capped)
    weights = exp_gate / lax.optimization_barrier(jnp.sum(exp_gate, axis=-1, keepdims=True))
    student = lax.optimization_barrier(jnp.sum(weights * flat_logits, axis=-1))
    residual_w = (student - target) * loss_scale
    d_gate = weights * (flat_logits - student[:, None]) * (1.0 - capped * capped)
    d_hidden = jnp.dot(d_gate, w_out.T, precision=lax.Precision.HIGHEST)
    d_pre = d_hidden * sig_pre * (1.0 + hidden_in * (1.0 - sig_pre))
    d_flat = residual_w[:, None] * (weights + jnp.dot(d_pre, w_in.T, precision=lax.Precision.HIGHEST))
    logit_gradient = (d_flat * reciprocal_norm).astype(jnp.bfloat16).reshape(mixture_logits.shape).astype(jnp.float32)
    user_gradient = jnp.einsum('ftz,fzr->ftr', logit_gradient, item_broadcast, precision=lax.Precision.HIGHEST)
    item_gradient = jnp.einsum('uwx,uwz->uxz', logit_gradient, user_broadcast, precision=lax.Precision.HIGHEST)
    return (user_gradient, item_gradient)

def reference(user_comps, item_text, item_proj, w_in, b_in, w_out, b_out, pair_user, pair_item, teacher):
    user_three = user_comps.reshape(USERS, COMPS, CDIM)
    mixed = jnp.dot(item_text, item_proj, preferred_element_type=jnp.float32).reshape(ITEMS, COMPS, CDIM)
    item_three = component_norm(mixed).astype(jnp.bfloat16)
    loss_scale = 2.0 * math.sqrt(USER_DEV / (PAIR_DEV * N_ITEM))
    tile_total = N_USER * N_ITEM
    user_ids = pair_user.reshape(tile_total, PAIR_DEV)
    item_ids = pair_item.reshape(tile_total, PAIR_DEV)
    targets = teacher.reshape(tile_total, PAIR_DEV)
    tile_ids = jnp.arange(tile_total, dtype=jnp.int32)

    def one_tile(sums, inputs):
        tile_id, local_user, local_item, target = inputs
        row_index = tile_id // N_ITEM
        col_index = tile_id % N_ITEM
        global_user = (row_index * USER_DEV + local_user).astype(jnp.int32)
        global_item = ((local_item // ISUB * N_ITEM + col_index) * ISUB + local_item % ISUB).astype(jnp.int32)
        user_gradient, item_gradient = pair_grads(user_three[global_user], item_three[global_item], target, w_in, b_in, w_out, b_out, loss_scale)
        return ((sums[0].at[global_user].add(user_gradient), sums[1].at[global_item].add(item_gradient)), None)
    start_sums = (jnp.zeros((USERS, COMPS, CDIM), jnp.float32), jnp.zeros((ITEMS, COMPS, CDIM), jnp.float32))
    (grad_users, grad_items), _ = lax.scan(one_tile, start_sums, (tile_ids, user_ids, item_ids, targets))
    return (grad_users.reshape(USERS, COMPS * CDIM), grad_items.reshape(ITEMS, COMPS * CDIM))
```

```python
import math

import jax
import jax.numpy as jnp
from jax import lax
from jax.experimental import pallas as pl
from jax.experimental.pallas import tpu as pltpu
from jax.sharding import PartitionSpec as P

MESH = pl.DeviceIdType.MESH
BF16 = jnp.bfloat16
F32 = jnp.float32

COMPS = 8
CDIM = 64
WIDE = COMPS * CDIM
GATES = 64
HIDDEN = 128
ROWS = 8
N_USER = 32
N_ITEM = 16
N_Z = 4
N_YC = 8
USERS = ROWS * N_ITEM
ITEMS = ROWS * N_USER
PAIRS = 1024
LANES = 128
CHUNKS = PAIRS // LANES
LOSS_SCALE = 2.0 * math.sqrt(USERS / (PAIRS * N_ITEM))
NT = (((1,), (1,)), ((), ()))
TN = (((0,), (0,)), ((), ()))


def dot(a, b, dims=(((1,), (0,)), ((), ()))):
    return lax.dot_general(a, b, dims, preferred_element_type=F32)


def split(x):
    upper = x.astype(BF16)
    return upper, (x - upper.astype(F32)).astype(BF16)


def store_parts(ref, x, lanes):
    n = x.shape[0]
    upper, lower = split(x)
    ref[0:n, lanes] = upper
    ref[n : 2 * n, lanes] = lower
    ref[2 * n : 3 * n, lanes] = upper


def chunk(g):
    return slice(g * LANES, (g + 1) * LANES)


def moving(g):
    return pl.ds(pl.multiple_of(g * LANES, LANES), LANES)


def kernel(
    uc_h, it_h, ip_h, win_h, bin_h, wout_h, bout_h, pu_h, pi_h, te_h,
    ug_o, ig_o,
    uc, it, ip, win, bin_, wout, bout, pu, pi, te,
    ubuf, ibuf, wot, bot, bcol, bocol, w1, w2, w3, w4,
    ohu, ohi, up, un, vn, logits, x1, x2, x3, x4, pre_r, sil_r, raw_r, wt_r, res_r, grad_r,
    igt, ugt, isum, usum, asend, abuf, bsend, bbuf, csend, cbuf,
    in_sem, zs, ys, us, isem, usem, as_, asem, bs, bsem, cs, csem,
):
    me_u = lax.axis_index("user")
    me_i = lax.axis_index("item")
    z = me_u // N_YC
    yc = me_u % N_YC

    barrier = pltpu.get_barrier_semaphore()

    def greet(a, b):
        pl.semaphore_signal(barrier, inc=1, device_id=(a, b), device_id_type=MESH)

    for o in (2, 1, 3):
        greet((z + o) % N_Z * N_YC + yc, me_i)
    for o in range(1, N_YC):
        greet(z * N_YC + (yc + o) % N_YC, me_i)
    for o in range(1, N_ITEM):
        greet(me_u, (me_i + o) % N_ITEM)

    pairs_in = [
        (ip_h, ip), (it_h, it), (uc_h, uc), (win_h, win), (bin_h, bin_), (wout_h, wout),
        (bout_h, bout), (pu_h, pu), (pi_h, pi), (te_h, te),
    ]
    loads = [pltpu.make_async_copy(s, d, in_sem.at[n]) for n, (s, d) in enumerate(pairs_in)]
    for load in loads:
        load.start()

    row = lax.broadcasted_iota(jnp.int32, (WIDE, WIDE), 0)
    col = lax.broadcasted_iota(jnp.int32, (WIDE, WIDE), 1)
    blocks = jnp.where(row // CDIM == col // CDIM, 1.0, 0.0).astype(BF16)
    loads[0].wait()
    loads[1].wait()
    mixed = dot(it[...], ip[...])
    upper, lower = split(mixed * mixed)
    square = dot(upper, blocks) + dot(lower, blocks)
    own_item = mixed * lax.rsqrt(square * (1.0 / CDIM) + 1e-06)
    ibuf[me_u] = own_item.astype(BF16)
    loads[2].wait()
    ubuf[me_i] = uc[...]

    pl.semaphore_wait(barrier, (N_Z - 1) + (N_YC - 1) + (N_ITEM - 1))

    def item_send(slot, peer, sem):
        return pltpu.make_async_remote_copy(
            src_ref=ibuf.at[slot], dst_ref=ibuf.at[slot], send_sem=sem, recv_sem=isem.at[slot],
            device_id=(peer, me_i), device_id_type=MESH,
        )

    sends = []
    for n, o in enumerate((2, 1, 3)):
        copy = item_send(me_u, (z + o) % N_Z * N_YC + yc, zs.at[n])
        copy.start()
        sends.append(copy)

    def pass_on(o):
        slot = (z + o) % N_Z * N_YC + yc
        for q in range(1, N_YC):
            copy = item_send(slot, z * N_YC + (yc + q) % N_YC, ys.at[o * N_YC + q])
            copy.start()
            sends.append(copy)

    pass_on(0)

    def user_send(slot, peer, sem):
        return pltpu.make_async_remote_copy(
            src_ref=ubuf.at[slot], dst_ref=ubuf.at[slot], send_sem=sem, recv_sem=usem.at[slot],
            device_id=(me_u, peer), device_id_type=MESH,
        )

    for o in range(1, N_ITEM):
        copy = user_send(me_i, (me_i + o) % N_ITEM, us.at[o])
        copy.start()
        sends.append(copy)

    for o in (1, 3):
        slot = (z + o) % N_Z * N_YC + yc
        item_send(slot, me_u, zs.at[0]).wait_recv()
        pass_on(o)

    for load in loads[3:]:
        load.wait()
    wot[...] = jnp.transpose(wout[...])
    bot[...] = jnp.transpose(jnp.broadcast_to(bout[...], (LANES, GATES)))
    bcol[...] = jnp.transpose(jnp.broadcast_to(bin_[...], (LANES, HIDDEN)))

    def reordered(ref):
        return jnp.concatenate([ref[pl.ds(k, COMPS, stride=COMPS), :] for k in range(COMPS)], axis=0)

    bocol[...] = reordered(bot)
    zeros = jnp.zeros((GATES, HIDDEN), F32)
    for source, tall, flat in ((win, w1, w4), (wot, w3, w2)):
        w = reordered(source)
        upper, lower = split(w)
        flat[:, 0:HIDDEN] = upper
        flat[:, HIDDEN : 2 * HIDDEN] = upper
        flat[:, 2 * HIDDEN : 3 * HIDDEN] = lower
        upper, lower = upper.astype(F32), lower.astype(F32)
        stacked = jnp.concatenate([upper, upper, lower, zeros], axis=0)
        tall[...] = jnp.transpose(stacked).astype(BF16)

    user_range = lax.broadcasted_iota(jnp.int32, (USERS, LANES), 0)
    item_range = lax.broadcasted_iota(jnp.int32, (ITEMS, LANES), 0)
    for g in range(CHUNKS):
        ohu[:, chunk(g)] = jnp.where(user_range == pu[g : g + 1, :], 1.0, 0.0).astype(BF16)
        ohi[:, chunk(g)] = jnp.where(item_range == pi[g : g + 1, :], 1.0, 0.0).astype(BF16)
    x1[3 * GATES :, :] = jnp.zeros((GATES, PAIRS), BF16)
    x3[3 * GATES :, :] = jnp.zeros((GATES, PAIRS), BF16)
    shuffle = jnp.where(col == row % CDIM * COMPS + row // CDIM, 1.0, 0.0).astype(BF16)

    slot = (z + 2) % N_Z * N_YC + yc
    item_send(slot, me_u, zs.at[0]).wait_recv()
    pass_on(2)

    for o in range(1, N_ITEM):
        user_send((me_i + o) % N_ITEM, me_i, us.at[0]).wait_recv()
    user_tile = ubuf[...].astype(F32).reshape(USERS, WIDE).astype(BF16)
    un[...] = dot(user_tile, ohu[...], TN)
    up[...] = dot(dot(user_tile, shuffle).astype(BF16), ohu[...], TN)

    for o in range(N_Z):
        for q in range(1, N_YC):
            item_send((z + o) % N_Z * N_YC + (yc + q) % N_YC, me_u, zs.at[0]).wait_recv()
    item_tile = ibuf[...].astype(F32).reshape(ITEMS, WIDE).astype(BF16)
    vn[...] = dot(item_tile, ohi[...], TN).reshape(vn.shape)

    def logit_chunk(g, _):
        lanes = moving(g)

        def step(block, total):
            total = list(total)
            for j in range(8):
                d = block * 8 + j
                u = up[pl.ds(pl.multiple_of(d * COMPS, COMPS), COMPS), lanes]
                for k in range(COMPS):
                    total[k] = total[k] + u * vn[k * 8 + block, j : j + 1, lanes]
            return tuple(total)

        total = lax.fori_loop(0, CDIM // 8, step, (jnp.zeros((COMPS, LANES), F32),) * COMPS)
        x = jnp.concatenate(total, axis=0) * (1.0 / math.sqrt(CDIM))
        logits[:, lanes] = x
        store_parts(x1, x, lanes)
        return 0

    lax.fori_loop(0, CHUNKS, logit_chunk, 0)

    pre_r[...] = dot(w1[...], x1[...])
    for g in range(CHUNKS):
        pre = pre_r[:, chunk(g)] + bcol[...]
        sig = 0.5 * jnp.tanh(0.5 * pre) + 0.5
        store_parts(x2, pre * sig, chunk(g))
        sil_r[:, chunk(g)] = sig * (1.0 + pre * (1.0 - sig))
    raw_r[...] = dot(w2[...], x2[...])
    for g in range(CHUNKS):
        capped = jnp.tanh((raw_r[:, chunk(g)] + bocol[...]) * 0.125)
        powers = jnp.exp(8.0 * capped)
        weights = powers * (1.0 / jnp.sum(powers, axis=0, keepdims=True))
        flat = logits[:, chunk(g)]
        student = jnp.sum(weights * flat, axis=0, keepdims=True)
        store_parts(x3, weights * (flat - student) * (1.0 - capped * capped), chunk(g))
        wt_r[:, chunk(g)] = weights
        res_r[g : g + 1, :] = (student - te[g : g + 1, :]) * LOSS_SCALE
    pre_r[...] = dot(w3[...], x3[...])
    for g in range(CHUNKS):
        store_parts(x4, pre_r[:, chunk(g)] * sil_r[:, chunk(g)], chunk(g))
    raw_r[...] = dot(w4[...], x4[...])
    for g in range(CHUNKS):
        d_flat = res_r[g : g + 1, :] * (wt_r[:, chunk(g)] + raw_r[:, chunk(g)])
        grad_r[:, chunk(g)] = (d_flat * (1.0 / math.sqrt(CDIM))).astype(BF16).astype(F32)

    def item_chunk(g, _):
        lanes = moving(g)
        for k in range(COMPS):
            total = None
            for c in range(COMPS):
                term = grad_r[k * COMPS + c : k * COMPS + c + 1, lanes] * un[c * CDIM : (c + 1) * CDIM, lanes]
                total = term if total is None else total + term
            igt[k * CDIM : (k + 1) * CDIM, lanes] = total.astype(BF16)
        return 0

    lax.fori_loop(0, CHUNKS, item_chunk, 0)
    isum[...] = dot(ohi[...], igt[...], NT).reshape(N_Z, N_YC, ROWS, WIDE)
    asend[...] = isum[...].astype(BF16)

    for o in range(1, N_YC):
        peer = (yc + o) % N_YC
        copy = pltpu.make_async_remote_copy(
            src_ref=asend.at[:, peer], dst_ref=abuf.at[yc], send_sem=as_.at[o], recv_sem=asem.at[yc],
            device_id=(z * N_YC + peer, me_i), device_id_type=MESH,
        )
        copy.start()
        sends.append(copy)

    def user_chunk(g, _):
        lanes = moving(g)
        for c in range(COMPS):
            total = None
            for k in range(COMPS):
                term = grad_r[k * COMPS + c : k * COMPS + c + 1, lanes] * vn[k * 8 : (k + 1) * 8, :, lanes].reshape(CDIM, LANES)
                total = term if total is None else total + term
            ugt[c * CDIM : (c + 1) * CDIM, lanes] = total.astype(BF16)
        return 0

    lax.fori_loop(0, CHUNKS, user_chunk, 0)
    usum[...] = dot(ohu[...], ugt[...], NT).reshape(N_ITEM, ROWS, WIDE)
    csend[...] = usum[...].astype(BF16)
    for o in range(1, N_ITEM):
        peer = (me_i + o) % N_ITEM
        copy = pltpu.make_async_remote_copy(
            src_ref=csend.at[peer], dst_ref=cbuf.at[me_i], send_sem=cs.at[o], recv_sem=csem.at[me_i],
            device_id=(me_u, peer), device_id_type=MESH,
        )
        copy.start()
        sends.append(copy)

    partial = isum[:, yc]
    for o in range(1, N_YC):
        peer = (yc + o) % N_YC
        pltpu.make_async_remote_copy(
            src_ref=abuf.at[peer], dst_ref=abuf.at[peer], send_sem=as_.at[0], recv_sem=asem.at[peer],
            device_id=(me_u, me_i), device_id_type=MESH,
        ).wait_recv()
        partial = partial + abuf[peer].astype(F32)
    bsend[...] = partial.astype(BF16)
    isum[:, 0] = partial
    for n, o in enumerate((2, 1, 3)):
        peer = (z + o) % N_Z
        copy = pltpu.make_async_remote_copy(
            src_ref=bsend.at[peer], dst_ref=bbuf.at[z], send_sem=bs.at[n], recv_sem=bsem.at[z],
            device_id=(peer * N_YC + yc, me_i), device_id_type=MESH,
        )
        copy.start()
        sends.append(copy)

    total = usum[me_i]
    for o in range(1, N_ITEM):
        peer = (me_i + o) % N_ITEM
        pltpu.make_async_remote_copy(
            src_ref=cbuf.at[peer], dst_ref=cbuf.at[peer], send_sem=cs.at[0], recv_sem=csem.at[peer],
            device_id=(me_u, me_i), device_id_type=MESH,
        ).wait_recv()
        total = total + cbuf[peer].astype(F32)
    ug_o[...] = total

    total = isum[z, 0]
    for o in (1, 3, 2):
        peer = (z + o) % N_Z
        pltpu.make_async_remote_copy(
            src_ref=bbuf.at[peer], dst_ref=bbuf.at[peer], send_sem=bs.at[0], recv_sem=bsem.at[peer],
            device_id=(me_u, me_i), device_id_type=MESH,
        ).wait_recv()
        total = total + bbuf[peer].astype(F32)
    ig_o[...] = total

    for copy in sends:
        copy.wait_send()


def local(
    user_comps, item_text, item_proj, w_in, b_in, w_out, b_out, pair_user, pair_item, teacher
):
    def vmem(shape, kind=F32):
        return pltpu.VMEM(shape, kind)

    inputs = (
        user_comps, item_text, item_proj, w_in, b_in.reshape(1, -1), w_out, b_out.reshape(1, -1),
        pair_user.reshape(CHUNKS, LANES), pair_item.reshape(CHUNKS, LANES), teacher.reshape(CHUNKS, LANES),
    )
    dma = pltpu.SemaphoreType.DMA
    scratch = [vmem(a.shape, a.dtype) for a in inputs] + [
        vmem((N_ITEM, ROWS, WIDE), BF16),
        vmem((N_USER, ROWS, WIDE), BF16),
        vmem((GATES, HIDDEN)),
        vmem((GATES, LANES)),
        vmem((HIDDEN, LANES)),
        vmem((GATES, LANES)),
        vmem((HIDDEN, 4 * GATES), BF16),
        vmem((GATES, 3 * HIDDEN), BF16),
        vmem((HIDDEN, 4 * GATES), BF16),
        vmem((GATES, 3 * HIDDEN), BF16),
        vmem((USERS, PAIRS), BF16),
        vmem((ITEMS, PAIRS), BF16),
        vmem((WIDE, PAIRS)),
        vmem((WIDE, PAIRS)),
        vmem((WIDE // 8, 8, PAIRS)),
        vmem((GATES, PAIRS)),
        vmem((4 * GATES, PAIRS), BF16),
        vmem((3 * HIDDEN, PAIRS), BF16),
        vmem((4 * GATES, PAIRS), BF16),
        vmem((3 * HIDDEN, PAIRS), BF16),
        vmem((HIDDEN, PAIRS)),
        vmem((HIDDEN, PAIRS)),
        vmem((GATES, PAIRS)),
        vmem((GATES, PAIRS)),
        vmem((CHUNKS, LANES)),
        vmem((GATES, PAIRS)),
        vmem((WIDE, PAIRS), BF16),
        vmem((WIDE, PAIRS), BF16),
        vmem((N_Z, N_YC, ROWS, WIDE)),
        vmem((N_ITEM, ROWS, WIDE)),
        vmem((N_Z, N_YC, ROWS, WIDE), BF16),
        vmem((N_YC, N_Z, ROWS, WIDE), BF16),
        vmem((N_Z, ROWS, WIDE), BF16),
        vmem((N_Z, ROWS, WIDE), BF16),
        vmem((N_ITEM, ROWS, WIDE), BF16),
        vmem((N_ITEM, ROWS, WIDE), BF16),
        dma((len(inputs),)),
        dma((N_Z,)),
        dma((N_Z * N_YC,)),
        dma((N_ITEM,)),
        dma((N_USER,)),
        dma((N_ITEM,)),
        dma((N_YC,)),
        dma((N_YC,)),
        dma((N_Z,)),
        dma((N_Z,)),
        dma((N_ITEM,)),
        dma((N_ITEM,)),
    ]
    out = jax.ShapeDtypeStruct((ROWS, WIDE), F32)
    return pl.pallas_call(
        kernel,
        out_shape=(out, out),
        in_specs=[pl.BlockSpec(memory_space=pl.ANY)] * len(inputs),
        out_specs=(pl.BlockSpec(memory_space=pltpu.VMEM),) * 2,
        scratch_shapes=scratch,
        compiler_params=pltpu.CompilerParams(
            collective_id=0, has_side_effects=True, vmem_limit_bytes=60 * 1024 * 1024
        ),
    )(*inputs)


def solution(mesh):
    split_both = P(("user", "item"), None)
    split_one = P(("user", "item"))
    in_specs = (
        split_both, split_both, P(), P(), P(), P(), P(), split_one, split_one, split_one,
    )
    return jax.shard_map(
        local, mesh=mesh, in_specs=in_specs, out_specs=(split_both, split_both), check_vma=False
    )
```

```python
import math

import jax
import jax.numpy as jnp
from jax import lax
from jax.experimental import pallas as pl
from jax.experimental.pallas import tpu as pltpu
from jax.sharding import PartitionSpec as P

MESH = pl.DeviceIdType.MESH
BF16 = jnp.bfloat16
F32 = jnp.float32

COMPS = 8
CDIM = 64
WIDE = COMPS * CDIM
GATES = 64
HIDDEN = 128
ROWS = 8
N_USER = 32
N_ITEM = 16
N_Z = 4
N_Y = 4
N_CORE = 2
N_YC = N_Y * N_CORE
N_X = 4
N_ZL = 4
HALF = COMPS // 2
SPAN = HALF * CDIM
PIECES = 4
PIECE = 1024 // PIECES
USERS = ROWS * N_ITEM
ITEMS = ROWS * N_USER
PAIRS = 1024
LANES = 128
CHUNKS = PAIRS // LANES
LOSS_SCALE = 2.0 * math.sqrt(USERS / (PAIRS * N_ITEM))
NT = (((1,), (1,)), ((), ()))
TN = (((0,), (0,)), ((), ()))


def dot(a, b, dims=(((1,), (0,)), ((), ()))):
    return lax.dot_general(a, b, dims, preferred_element_type=F32)


def split(x):
    upper = x.astype(BF16)
    return upper, (x - upper.astype(F32)).astype(BF16)


def store_parts(ref, x, lanes):
    n = x.shape[0]
    upper, lower = split(x)
    ref[0:n, lanes] = upper
    ref[n : 2 * n, lanes] = lower
    ref[2 * n : 3 * n, lanes] = upper


def chunk(g):
    return slice(g * LANES, (g + 1) * LANES)


def moving(g):
    return pl.ds(pl.multiple_of(g * LANES, LANES), LANES)


def kernel(
    uc_h, it_h, ip_h, win_h, bin_h, wout_h, bout_h, pu_h, pi_h, te_h,
    both_o,
    uc, it, ip, win, bin_, wout, bout, pu, pi, te,
    ubuf, ibuf, bot, bcol, bocol, w1, w2, w3, w4,
    ohu, ohi, up, un, vn, logits, x1, x2, x3, x4, pre_r, sil_r, raw_r, wt_r, res_r, grad_r,
    igt, ugt, isum, usum, iown, uown, asend, abuf, bsend, bbuf, csend, cbuf, dsend, dbuf,
    in_sem, zs, ys, us, isem, usem, as_, asem, bs, bsem, cs, csem, ds_, dsem,
):
    me_u = lax.axis_index("user")
    me_i = lax.axis_index("item")
    z, yc = me_u // N_YC, me_u % N_YC
    y, core = yc // N_CORE, yc % N_CORE
    x, zl = me_i // N_ZL, me_i % N_ZL

    group = [
        (y + dy) % N_Y * N_CORE + (core + dc) % N_CORE
        for dy in (2, 1, 3, 0) for dc in range(N_CORE) if dy or dc
    ]
    z_right, z_left, z_far = ((z + o) % N_Z for o in (1, 3, 2))
    zl_peers = [(zl + o) % N_ZL for o in range(1, N_ZL)]
    x_peers = [(x + o) % N_X for o in (2, 1, 3)]

    pieces = [(ip_h.at[pl.ds(n * PIECE, PIECE)], ip.at[pl.ds(n * PIECE, PIECE)]) for n in range(PIECES)]
    pairs_in = [(it_h, it)] + pieces + [
        (uc_h, uc), (win_h, win), (bin_h, bin_), (wout_h, wout),
        (bout_h, bout), (pu_h, pu), (pi_h, pi), (te_h, te),
    ]
    loads = [pltpu.make_async_copy(s, d, in_sem.at[n]) for n, (s, d) in enumerate(pairs_in)]
    for load in loads:
        load.start()

    barrier = pltpu.get_barrier_semaphore()

    def greet(a, b):
        pl.semaphore_signal(barrier, inc=1, device_id=(a, b), device_id_type=MESH)

    for a in (z_right, z_left):
        greet(a * N_YC + yc, me_i)
    for a in group:
        greet(z * N_YC + a, me_i)
    for b in zl_peers:
        greet(me_u, x * N_ZL + b)
    for b in x_peers:
        greet(me_u, b * N_ZL + zl)

    row = lax.broadcasted_iota(jnp.int32, (WIDE, WIDE), 0)
    col = lax.broadcasted_iota(jnp.int32, (WIDE, WIDE), 1)
    blocks = jnp.where(row // CDIM == col // CDIM, 1.0, 0.0).astype(BF16)
    loads[0].wait()
    mixed = None
    for n in range(PIECES):
        loads[1 + n].wait()
        part = dot(it[:, n * PIECE : (n + 1) * PIECE], ip[n * PIECE : (n + 1) * PIECE, :])
        mixed = part if mixed is None else mixed + part
    upper, lower = split(mixed * mixed)
    square = dot(upper, blocks) + dot(lower, blocks)
    own_item = mixed * lax.rsqrt(square * (1.0 / CDIM) + 1e-06)
    ibuf[me_u] = own_item.astype(BF16)
    loads[1 + PIECES].wait()
    ubuf[me_i] = uc[...]

    pl.semaphore_wait(barrier, 2 + (N_YC - 1) + (N_ZL - 1) + (N_X - 1))

    sends = []

    def send(src, dst, send_sem, recv_sem, a, b):
        copy = pltpu.make_async_remote_copy(
            src_ref=src, dst_ref=dst, send_sem=send_sem, recv_sem=recv_sem,
            device_id=(a, b), device_id_type=MESH,
        )
        copy.start()
        sends.append(copy)

    def arrived(dst, recv_sem):
        pltpu.make_async_remote_copy(
            src_ref=dst, dst_ref=dst, send_sem=zs.at[0], recv_sem=recv_sem,
            device_id=(me_u, me_i), device_id_type=MESH,
        ).wait_recv()

    def item_send(slot, peer, sem):
        send(ibuf.at[slot], ibuf.at[slot], sem, isem.at[slot], peer, me_i)

    def item_arrived(slot):
        arrived(ibuf.at[slot], isem.at[slot])

    def pass_on(source, n):
        for q, a in enumerate(group):
            item_send(source * N_YC + yc, z * N_YC + a, ys.at[n * N_YC + q])

    def user_send(slot, peer, sem):
        send(ubuf.at[slot], ubuf.at[slot], sem, usem.at[slot], me_u, peer)

    def user_arrived(slot):
        arrived(ubuf.at[slot], usem.at[slot])

    item_send(me_u, z_right * N_YC + yc, zs.at[0])
    item_send(me_u, z_left * N_YC + yc, zs.at[1])
    for n, b in enumerate(zl_peers):
        user_send(me_i, x * N_ZL + b, us.at[n])
    pass_on(z, 0)

    def user_pass_on(slot, n):
        for q, b in enumerate(x_peers):
            user_send(slot, b * N_ZL + zl, us.at[n * N_X + q])

    user_pass_on(me_i, 1)

    item_arrived(z_left * N_YC + yc)
    item_send(z_left * N_YC + yc, z_right * N_YC + yc, zs.at[2])
    pass_on(z_left, 1)
    for n, b in enumerate(zl_peers):
        user_arrived(x * N_ZL + b)
        user_pass_on(x * N_ZL + b, 2 + n)
    item_arrived(z_right * N_YC + yc)
    pass_on(z_right, 2)

    for load in loads[2 + PIECES :]:
        load.wait()
    bot[...] = jnp.transpose(jnp.broadcast_to(bout[...], (LANES, GATES)))
    bcol[...] = jnp.transpose(jnp.broadcast_to(bin_[...], (LANES, HIDDEN)))

    def reordered(ref):
        return jnp.concatenate([ref[pl.ds(k, COMPS, stride=COMPS), :] for k in range(COMPS)], axis=0)

    bocol[...] = reordered(bot)
    zeros = jnp.zeros((GATES, HIDDEN), F32)
    for source, tall, flat in ((win, w1, w4), (wout, w3, w2)):
        w = reordered(source)
        upper, lower = split(w)
        flat[:, 0:HIDDEN] = upper
        flat[:, HIDDEN : 2 * HIDDEN] = upper
        flat[:, 2 * HIDDEN : 3 * HIDDEN] = lower
        upper, lower = upper.astype(F32), lower.astype(F32)
        stacked = jnp.concatenate([upper, upper, lower, zeros], axis=0)
        tall[...] = jnp.transpose(stacked).astype(BF16)

    user_range = lax.broadcasted_iota(jnp.int32, (USERS, LANES), 0)
    item_range = lax.broadcasted_iota(jnp.int32, (ITEMS, LANES), 0)
    for g in range(CHUNKS):
        ohu[:, chunk(g)] = jnp.where(user_range == pu[g : g + 1, :], 1.0, 0.0).astype(BF16)
        ohi[:, chunk(g)] = jnp.where(item_range == pi[g : g + 1, :], 1.0, 0.0).astype(BF16)
    x1[3 * GATES :, :] = jnp.zeros((GATES, PAIRS), BF16)
    x3[3 * GATES :, :] = jnp.zeros((GATES, PAIRS), BF16)
    shuffle = jnp.where(col == row % CDIM * COMPS + row // CDIM, 1.0, 0.0).astype(BF16)

    item_arrived(z_far * N_YC + yc)
    pass_on(z_far, 3)

    for a in x_peers:
        for b in range(N_ZL):
            user_arrived(a * N_ZL + b)
    user_tile = ubuf[...].astype(F32).reshape(USERS, WIDE).astype(BF16)
    un[...] = dot(user_tile, ohu[...], TN)
    up[...] = dot(dot(user_tile, shuffle).astype(BF16), ohu[...], TN)

    for a in (z, z_left, z_right, z_far):
        for b in group:
            item_arrived(a * N_YC + b)
    item_tile = ibuf[...].astype(F32).reshape(ITEMS, WIDE).astype(BF16)
    vn[...] = dot(item_tile, ohi[...], TN).reshape(vn.shape)

    def logit_chunk(g, _):
        lanes = moving(g)

        total = [jnp.zeros((COMPS, LANES), F32)] * COMPS
        for d in range(CDIM):
            u = up[d * COMPS : (d + 1) * COMPS, lanes]
            for k in range(COMPS):
                total[k] = total[k] + u * vn[k * 8 + d // 8, d % 8 : d % 8 + 1, lanes]
        flat = jnp.concatenate(total, axis=0) * (1.0 / math.sqrt(CDIM))
        logits[:, lanes] = flat
        store_parts(x1, flat, lanes)
        return 0

    lax.fori_loop(0, CHUNKS, logit_chunk, 0)

    pre_r[...] = dot(w1[...], x1[...])
    for g in range(CHUNKS):
        pre = pre_r[:, chunk(g)] + bcol[...]
        sig = 0.5 * jnp.tanh(0.5 * pre) + 0.5
        store_parts(x2, pre * sig, chunk(g))
        sil_r[:, chunk(g)] = sig * (1.0 + pre * (1.0 - sig))
    raw_r[...] = dot(w2[...], x2[...])
    for g in range(CHUNKS):
        capped = jnp.tanh((raw_r[:, chunk(g)] + bocol[...]) * 0.125)
        powers = jnp.exp(8.0 * capped)
        weights = powers * (1.0 / jnp.sum(powers, axis=0, keepdims=True))
        flat = logits[:, chunk(g)]
        student = jnp.sum(weights * flat, axis=0, keepdims=True)
        store_parts(x3, weights * (flat - student) * (1.0 - capped * capped), chunk(g))
        wt_r[:, chunk(g)] = weights
        res_r[g : g + 1, :] = (student - te[g : g + 1, :]) * LOSS_SCALE
    pre_r[...] = dot(w3[...], x3[...])
    for g in range(CHUNKS):
        store_parts(x4, pre_r[:, chunk(g)] * sil_r[:, chunk(g)], chunk(g))
    raw_r[...] = dot(w4[...], x4[...])
    for g in range(CHUNKS):
        d_flat = res_r[g : g + 1, :] * (wt_r[:, chunk(g)] + raw_r[:, chunk(g)])
        grad_r[:, chunk(g)] = (d_flat * (1.0 / math.sqrt(CDIM))).astype(BF16).astype(F32)

    def expand(out, base, pick, values):
        def step(g, _):
            lanes = moving(g)
            factors = [
                [jnp.broadcast_to(grad_r[pick(i, j) : pick(i, j) + 1, lanes], (8, LANES)) for i in range(COMPS)]
                for j in range(HALF)
            ]
            for block in range(0, 8, 2):
                sums = [[], []]
                for n in range(2):
                    terms = [values(i, block + n, lanes) for i in range(COMPS)]
                    for j in range(HALF):
                        products = [f * t for f, t in zip(factors[j], terms)]
                        while len(products) > 1:
                            products = [a + b for a, b in zip(products[::2], products[1::2])]
                        sums[n].append(products[0])
                for j in range(HALF):
                    start = base + j * CDIM + block * 8
                    out[start : start + 16, lanes] = jnp.concatenate([sums[0][j], sums[1][j]], axis=0).astype(BF16)
            return 0

        lax.fori_loop(0, CHUNKS, step, 0)

    def item_values(c, block, lanes):
        return un[c * CDIM + block * 8 : c * CDIM + block * 8 + 8, lanes]

    for h in range(2):
        expand(igt, h * SPAN, lambda c, j: (h * HALF + j) * COMPS + c, item_values)
        part = dot(ohi[...], igt[h * SPAN : (h + 1) * SPAN, :], NT).reshape(N_Z, N_YC, ROWS, SPAN)
        isum[h] = part
        asend[h] = part.astype(BF16)
        for q, a in enumerate(group):
            send(
                asend.at[h, :, a], abuf.at[h, yc], as_.at[h * N_YC + q], asem.at[h * N_YC + yc],
                z * N_YC + a, me_i,
            )

    def user_values(k, block, lanes):
        return vn[k * 8 + block, :, lanes]

    for h in range(2):
        expand(ugt, h * SPAN, lambda k, j: k * COMPS + h * HALF + j, user_values)
    usum[...] = dot(ohu[...], ugt[...], NT).reshape(N_X, N_ZL, ROWS, WIDE)
    csend[...] = usum[...].astype(BF16)
    for q, b in enumerate(x_peers):
        send(csend.at[b], cbuf.at[x], cs.at[q], csem.at[x], me_u, b * N_ZL + zl)

    for h in range(2):
        total = isum[h, :, yc]
        for a in group[::-1]:
            arrived(abuf.at[h, a], asem.at[h * N_YC + a])
            total = total + abuf[h, a].astype(F32)
        bsend[h] = total.astype(BF16)
        iown[h] = total
        for q, a in enumerate((z_far, z_right, z_left)):
            send(
                bsend.at[h, a], bbuf.at[h, z], bs.at[h * N_Z + q], bsem.at[h * N_Z + z],
                a * N_YC + yc, me_i,
            )

    total = usum[x]
    for b in x_peers[::-1]:
        arrived(cbuf.at[b], csem.at[b])
        total = total + cbuf[b].astype(F32)
    dsend[...] = total.astype(BF16)
    uown[...] = total
    for q, b in enumerate(zl_peers):
        send(dsend.at[b], dbuf.at[zl], ds_.at[q], dsem.at[zl], me_u, x * N_ZL + b)
    total = uown[zl]
    for b in zl_peers:
        arrived(dbuf.at[b], dsem.at[b])
        total = total + dbuf[b].astype(F32)
    both_o[0] = total

    for h in range(2):
        total = iown[h, z]
        for a in (z_right, z_left, z_far):
            arrived(bbuf.at[h, a], bsem.at[h * N_Z + a])
            total = total + bbuf[h, a].astype(F32)
        both_o[1, :, h * SPAN : (h + 1) * SPAN] = total

    for copy in sends:
        copy.wait_send()


def local(
    user_comps, item_text, item_proj, w_in, b_in, w_out, b_out, pair_user, pair_item, teacher
):
    def vmem(shape, kind=F32):
        return pltpu.VMEM(shape, kind)

    inputs = (
        user_comps, item_text, item_proj, w_in, b_in.reshape(1, -1), w_out.T, b_out.reshape(1, -1),
        pair_user.reshape(CHUNKS, LANES), pair_item.reshape(CHUNKS, LANES), teacher.reshape(CHUNKS, LANES),
    )
    dma = pltpu.SemaphoreType.DMA
    scratch = [vmem(a.shape, a.dtype) for a in inputs] + [
        vmem((N_ITEM, ROWS, WIDE), BF16),
        vmem((N_USER, ROWS, WIDE), BF16),
        vmem((GATES, LANES)),
        vmem((HIDDEN, LANES)),
        vmem((GATES, LANES)),
        vmem((HIDDEN, 4 * GATES), BF16),
        vmem((GATES, 3 * HIDDEN), BF16),
        vmem((HIDDEN, 4 * GATES), BF16),
        vmem((GATES, 3 * HIDDEN), BF16),
        vmem((USERS, PAIRS), BF16),
        vmem((ITEMS, PAIRS), BF16),
        vmem((WIDE, PAIRS)),
        vmem((WIDE, PAIRS)),
        vmem((WIDE // 8, 8, PAIRS)),
        vmem((GATES, PAIRS)),
        vmem((4 * GATES, PAIRS), BF16),
        vmem((3 * HIDDEN, PAIRS), BF16),
        vmem((4 * GATES, PAIRS), BF16),
        vmem((3 * HIDDEN, PAIRS), BF16),
        vmem((HIDDEN, PAIRS)),
        vmem((HIDDEN, PAIRS)),
        vmem((GATES, PAIRS)),
        vmem((GATES, PAIRS)),
        vmem((CHUNKS, LANES)),
        vmem((GATES, PAIRS)),
        vmem((WIDE, PAIRS), BF16),
        vmem((WIDE, PAIRS), BF16),
        vmem((2, N_Z, N_YC, ROWS, SPAN)),
        vmem((N_X, N_ZL, ROWS, WIDE)),
        vmem((2, N_Z, ROWS, SPAN)),
        vmem((N_ZL, ROWS, WIDE)),
        vmem((2, N_Z, N_YC, ROWS, SPAN), BF16),
        vmem((2, N_YC, N_Z, ROWS, SPAN), BF16),
        vmem((2, N_Z, ROWS, SPAN), BF16),
        vmem((2, N_Z, ROWS, SPAN), BF16),
        vmem((N_X, N_ZL, ROWS, WIDE), BF16),
        vmem((N_X, N_ZL, ROWS, WIDE), BF16),
        vmem((N_ZL, ROWS, WIDE), BF16),
        vmem((N_ZL, ROWS, WIDE), BF16),
        dma((len(inputs) - 1 + PIECES,)),
        dma((N_Z,)),
        dma((N_Z * N_YC,)),
        dma(((N_ZL + 1) * N_X,)),
        dma((N_USER,)),
        dma((N_ITEM,)),
        dma((2 * N_YC,)),
        dma((2 * N_YC,)),
        dma((2 * N_Z,)),
        dma((2 * N_Z,)),
        dma((N_X,)),
        dma((N_X,)),
        dma((N_ZL,)),
        dma((N_ZL,)),
    ]
    both = pl.pallas_call(
        kernel,
        out_shape=pltpu.VMEM((2, ROWS, WIDE), F32),
        in_specs=[pl.BlockSpec(memory_space=pl.ANY)] * len(inputs),
        out_specs=pl.BlockSpec(memory_space=pltpu.VMEM),
        scratch_shapes=scratch,
        compiler_params=pltpu.CompilerParams(
            collective_id=0, has_side_effects=True, vmem_limit_bytes=60 * 1024 * 1024
        ),
    )(*inputs)
    return both[0], both[1]


def solution(mesh):
    split_both = P(("user", "item"), None)
    split_one = P(("user", "item"))
    in_specs = (
        split_both, split_both, P(), P(), P(), P(), P(), split_one, split_one, split_one,
    )
    return jax.shard_map(
        local, mesh=mesh, in_specs=in_specs, out_specs=(split_both, split_both), check_vma=False
    )
```
